32 devices in a mesh: gx: 8 (over z, core), gy: 4 (over y, x).
Axes of the slice: x: 2, y: 2, z: 4, core: 2. Of those that a mesh axis runs over, the one named last changes fastest.
Arguments:
- density: float32 [128, 64, 128], P('gx', 'gy'), may hold values from 0.05 to 40, as said below
Outputs:
- potential: float32 [128, 64, 128], P('gx', 'gy')
The draws below stay inside these ranges and needn't reach their ends.
Inputs may be any that keep to these rules, and one draw needn't show every extreme that they name: `density`: densities are positive.
All inputs are finite; a program needn't handle non-finite values.
Results may differ from the reference program's by a relative error of at most 0.00014.
Values sent between devices are 32-bit elements; how exact they have to be, the bound alone decides.
A program may use at most 64 MiB of HBM per device.

```python
import jax
import jax.numpy as jnp

LEVELS = 4
NEWTON = 3
COARSE_SWEEPS = 2
NX = 128
NY = 64
NZ = 128


def draw_density(key, part):
    noise_key = jax.random.fold_in(jax.random.fold_in(key, 17), 0)
    noise_draw = jnp.clip(jax.random.normal(noise_key, (NX, NY, NZ), jnp.float32), -4.0, 4.0)
    coord_x = jnp.arange(NX, dtype=jnp.float32) / NX
    coord_y = jnp.arange(NY, dtype=jnp.float32) / NY
    tilt_factor = (1.0 + coord_x)[:, None, None] * (1.0 + coord_y)[None, :, None]
    density_field = jnp.exp(0.3 * noise_draw) * tilt_factor
    return density_field.astype(jnp.float32)


def setup_inputs(seed: int = 0) -> dict:
    key_of = jax.random.split(jax.random.key(seed), 2)
    return {
        "density": draw_density(jax.random.fold_in(key_of[1], 71), 0),
    }


COUPLING = 0.1
FLOOR = 3.0


def shifted(padded, off_x, off_y, off_z):
    size_x = padded.shape[0] - 2
    size_y = padded.shape[1] - 2
    size_z = padded.shape[2] - 2
    return padded[1 + off_x:1 + off_x + size_x, 1 + off_y:1 + off_y + size_y, 1 + off_z:1 + off_z + size_z]


def hessian(padded, spacing_inv):
    center = shifted(padded, 0, 0, 0)
    pure_x = (shifted(padded, 1, 0, 0) + shifted(padded, -1, 0, 0) - 2.0 * center) * spacing_inv
    pure_y = (shifted(padded, 0, 1, 0) + shifted(padded, 0, -1, 0) - 2.0 * center) * spacing_inv
    pure_z = (shifted(padded, 0, 0, 1) + shifted(padded, 0, 0, -1) - 2.0 * center) * spacing_inv
    quarter = 0.25 * spacing_inv
    mixed_xy = (shifted(padded, 1, 1, 0) - shifted(padded, 1, -1, 0) - shifted(padded, -1, 1, 0) + shifted(padded, -1, -1, 0)) * quarter
    mixed_xz = (shifted(padded, 1, 0, 1) - shifted(padded, 1, 0, -1) - shifted(padded, -1, 0, 1) + shifted(padded, -1, 0, -1)) * quarter
    mixed_yz = (shifted(padded, 0, 1, 1) - shifted(padded, 0, 1, -1) - shifted(padded, 0, -1, 1) + shifted(padded, 0, -1, -1)) * quarter
    return pure_x, pure_y, pure_z, mixed_xy, mixed_xz, mixed_yz


def nonlinear(padded, source):
    pure_x, pure_y, pure_z, mixed_xy, mixed_xz, mixed_yz = hessian(padded, 1.0)
    cubic = 2.0 * (pure_x * pure_y + pure_x * pure_z + pure_y * pure_z - mixed_xy * mixed_xy - mixed_xz * mixed_xz - mixed_yz * mixed_yz)
    return pure_x + pure_y + pure_z + COUPLING * cubic - source


def coefficients(padded, spacing_inv):
    pure_x, pure_y, pure_z, mixed_xy, mixed_xz, mixed_yz = hessian(padded, spacing_inv)
    stiff_x = 1.0 + 2.0 * COUPLING * (pure_y + pure_z)
    stiff_y = 1.0 + 2.0 * COUPLING * (pure_x + pure_z)
    stiff_z = 1.0 + 2.0 * COUPLING * (pure_x + pure_y)
    diagonal = jnp.maximum(2.0 * (stiff_x + stiff_y + stiff_z), FLOOR)
    relax = 1.0 / (spacing_inv * diagonal)
    return jnp.stack([stiff_x, stiff_y, stiff_z, -4.0 * COUPLING * mixed_xy, -4.0 * COUPLING * mixed_xz, -4.0 * COUPLING * mixed_yz, relax])


def jacobian(padded, weights, spacing_inv):
    parts = hessian(padded, spacing_inv)
    result = weights[0] * parts[0]
    for index in range(1, 6):
        result = result + weights[index] * parts[index]
    return result


def restrict(field):
    size_x, size_y, size_z = field.shape
    blocks = field.reshape(size_x // 2, 2, size_y // 2, 2, size_z // 2, 2)
    return jnp.sum(blocks, axis=(1, 3, 5)) * 0.125


def prolong(field):
    size_x, size_y, size_z = field.shape
    spread = jnp.broadcast_to(field[:, None, :, None, :, None], (size_x, 2, size_y, 2, size_z, 2))
    return spread.reshape(2 * size_x, 2 * size_y, 2 * size_z)


def wrap_all(field):
    return jnp.pad(field, 1, mode="wrap")


def checker(shape, first_x, first_y, first_z):
    index_x = first_x + jnp.arange(shape[0], dtype=jnp.int32)
    index_y = first_y + jnp.arange(shape[1], dtype=jnp.int32)
    index_z = first_z + jnp.arange(shape[2], dtype=jnp.int32)
    parity = (index_x[:, None, None] + index_y[None, :, None] + index_z[None, None, :]) % 2
    return (parity == 0).astype(jnp.float32)


def black_half(change, target, weights, red_mask, extend, spacing_inv):
    black_mask = 1.0 - red_mask
    return change + black_mask * (jacobian(extend(change), weights, spacing_inv) - target) * weights[6]


def first_sweep(target, weights, red_mask, extend, spacing_inv):
    change = -red_mask * target * weights[6]
    return black_half(change, target, weights, red_mask, extend, spacing_inv)


def full_sweep(change, target, weights, red_mask, extend, spacing_inv):
    change = change + red_mask * (jacobian(extend(change), weights, spacing_inv) - target) * weights[6]
    return black_half(change, target, weights, red_mask, extend, spacing_inv)


def cycle(coarse_level, target, weight_levels, mask_levels):
    spacing_inv = 0.25 ** coarse_level
    weights = weight_levels[coarse_level]
    red_mask = mask_levels[coarse_level]
    change = first_sweep(target, weights, red_mask, wrap_all, spacing_inv)
    if coarse_level == LEVELS - 1:
        for repeat in range(COARSE_SWEEPS - 1):
            change = full_sweep(change, target, weights, red_mask, wrap_all, spacing_inv)
        return change
    leftover = target - jacobian(wrap_all(change), weights, spacing_inv)
    change = change + prolong(cycle(coarse_level + 1, restrict(leftover), weight_levels, mask_levels))
    return full_sweep(change, target, weights, red_mask, wrap_all, spacing_inv)


def reference(density):
    source = density / (jnp.sum(density) / density.size) - 1.0
    potential = jnp.zeros_like(density)
    for newton_step in range(NEWTON):
        weight_levels = []
        mask_levels = []
        coarse = potential
        target = source
        for coarse_level in range(LEVELS):
            if coarse_level > 0:
                coarse = restrict(coarse)
            padded = wrap_all(coarse)
            if coarse_level == 0:
                target = -nonlinear(padded, source)
            weight_levels.append(coefficients(padded, 0.25 ** coarse_level))
            mask_levels.append(checker(coarse.shape, 0, 0, 0))
        potential = potential + cycle(0, target, weight_levels, mask_levels)
    return potential
```

```python
import functools

import jax
import jax.numpy as jnp
from jax import lax
from jax.experimental import pallas as pl
from jax.experimental.pallas import tpu as pltpu
from jax.sharding import PartitionSpec as P

LEVELS = 4
NEWTON = 3
COUPLING = 0.1
FLOOR = 3.0
HALO = 8
MESH = pl.DeviceIdType.MESH


def parts_of(block, step):
    rows, lanes = block.shape[1], block.shape[2]
    center = block[1:-1]
    twice = center + center
    z_next = pltpu.roll(block, lanes - step, 2)
    z_prev = pltpu.roll(block, step, 2)
    y_next = pltpu.roll(block, rows - 1, 1)
    y_prev = pltpu.roll(block, 1, 1)
    slope_z = z_next - z_prev
    slope_y = y_next - y_prev
    xx = block[2:] + block[:-2] - twice
    yy = y_next[1:-1] + y_prev[1:-1] - twice
    zz = z_next[1:-1] + z_prev[1:-1] - twice
    xy = slope_y[2:] - slope_y[:-2]
    xz = slope_z[2:] - slope_z[:-2]
    inner = slope_z[1:-1]
    yz = pltpu.roll(inner, rows - 1, 1) - pltpu.roll(inner, 1, 1)
    return center, xx, yy, zz, xy, xz, yz


def red_of(shape, first, level):
    total = (
        lax.broadcasted_iota(jnp.int32, shape, 0)
        + first
        + lax.broadcasted_iota(jnp.int32, shape, 1)
        + (lax.broadcasted_iota(jnp.int32, shape, 2) >> level)
    )
    return (total & 1) == 0


def planes(first, count, body):
    size = 4 if count % 4 == 0 else 2
    assert count % size == 0

    def turn(i, carry):
        body(first + i * size, size)
        return carry

    lax.fori_loop(0, count // size, turn, 0)


class Level:
    def __init__(self, level, pad, weights, target, va, vb):
        self.level, self.pad = level, pad
        self.weights, self.target, self.va, self.vb = weights, target, va, vb
        self.step = 1 << level
        self.scale = 0.25**level

    def setup(self, u_ref, first, count, source_ref=None):
        def body(at, size):
            block = u_ref[pl.ds(at - 1, size + 2)]
            _, xx, yy, zz, xy, xz, yz = parts_of(block, self.step)
            if self.level > 0:
                xx, yy, zz = xx * self.scale, yy * self.scale, zz * self.scale
            quarter = 0.25 * self.scale
            xy, xz, yz = xy * quarter, xz * quarter, yz * quarter
            kx = 1.0 + 2.0 * COUPLING * (yy + zz)
            ky = 1.0 + 2.0 * COUPLING * (xx + zz)
            kz = 1.0 + 2.0 * COUPLING * (xx + yy)
            diagonal = jnp.maximum(2.0 * (kx + ky + kz), FLOOR)
            relax = 1.0 / (self.scale * diagonal)
            rows = pl.ds(at, size)
            if source_ref is not None:
                cubic = 2.0 * (xx * yy + xx * zz + yy * zz - xy * xy - xz * xz - yz * yz)
                target = source_ref[rows] - (xx + yy + zz + COUPLING * cubic)
                self.target[rows] = target
            else:
                target = self.target[rows]
            mixed = -4.0 * COUPLING * quarter
            self.weights[0, rows] = kx * self.scale
            self.weights[1, rows] = ky * self.scale
            self.weights[2, rows] = kz * self.scale
            self.weights[3, rows] = xy * mixed
            self.weights[4, rows] = xz * mixed
            self.weights[5, rows] = yz * mixed
            self.weights[6, rows] = relax
            red = red_of(target.shape, (first - self.pad) % 2, self.level)
            self.va[rows] = jnp.where(red, -target * relax, 0.0)

        planes(first, count, body)

    def excess(self, v_ref, at, size):
        block = v_ref[pl.ds(at - 1, size + 2)]
        center, xx, yy, zz, xy, xz, yz = parts_of(block, self.step)
        rows = pl.ds(at, size)
        w = self.weights
        total = w[0, rows] * xx + w[1, rows] * yy + w[2, rows] * zz
        total += w[3, rows] * xy + w[4, rows] * xz + w[5, rows] * yz
        return total - self.target[rows], center

    def half(self, src, first, count, red, put):
        def body(at, size):
            excess, center = self.excess(src, at, size)
            change = excess * self.weights[6, pl.ds(at, size)]
            mask = red_of(change.shape, (first - self.pad) % 2, self.level)
            if red:
                value = jnp.where(mask, center + change, center)
            else:
                value = jnp.where(mask, center, center + change)
            put(at, size, value)

        planes(first, count, body)


def store_to(ref):
    def put(at, size, value):
        ref[pl.ds(at, size)] = value

    return put


def pair_xz(value, step):
    size, rows, lanes = value.shape
    halves = value.reshape(size // 2, 2, rows, lanes)
    value = halves[:, 0] + halves[:, 1]
    lane = lax.broadcasted_iota(jnp.int32, value.shape, 2)
    other = jnp.where(
        (lane & step) == 0, pltpu.roll(value, lanes - step, 2), pltpu.roll(value, step, 2)
    )
    return value + other


def pair_y(tmp, first, count, rows, out, out_first, out_row):
    half = rows // 2

    def body(i, carry):
        low = tmp[first + i, pl.ds(0, half, stride=2), :]
        high = tmp[first + i, pl.ds(1, half, stride=2), :]
        out[out_first + i, pl.ds(out_row, half), :] = (low + high) * 0.125
        return carry

    lax.fori_loop(0, count, body, 0)


def wrap_planes(ref, pad, count):
    for i in range(pad):
        ref[i] = ref[count + i]
        ref[pad + count + i] = ref[pad + i]


def kernel(
    gx, gy, density_ref, out_ref,
    S, U, W0, T0, A0, B0, R0,
    U1, W1, T1, A1, B1, X1, R1,
    U2, W2, T2, A2, B2, R2,
    U3, W3, T3, A3, B3,
    G,
    near_send, near_recv, mid_send, mid_recv, row_send, row_recv, col_send, col_recv,
):
    bx, by, nz = density_ref.shape
    me_x, me_y = lax.axis_index("gx"), lax.axis_index("gy")
    pad1 = HALO // 2
    b1x, b1y = bx // 2, by // 2
    b2x, b2y = bx // 4, by // 4
    n2x, n2y = b2x * gx, b2y * gy
    n3x, n3y = n2x // 2, n2y // 2
    row1 = HALO

    def device(dx, dy):
        return (lax.rem(me_x + dx + gx, gx), lax.rem(me_y + dy + gy, gy))

    around = [(dx, dy) for dx in (-1, 0, 1) for dy in (-1, 0, 1) if (dx, dy) != (0, 0)]
    friends = [device(d, 0) for d in range(1, gx)]
    friends += [device(0, d) for d in range(1, gy)]
    friends += [device(dx, dy) for dx, dy in around if dx and dy]
    barrier = pltpu.get_barrier_semaphore()
    for friend in friends:
        pl.semaphore_signal(barrier, inc=1, device_id=friend, device_id_type=MESH)
    pl.semaphore_wait(barrier, len(friends))

    def spans(d, block, halo):
        if d == 0:
            return (halo, halo, block)
        if d == 1:
            return (block, 0, halo)
        return (halo, block + halo, halo)

    def exchange(ref, block_x, halo_x, block_y, halo_y, send, recv, turn):
        copies = []
        for index, (dx, dy) in enumerate(around):
            sx, rx, cx = spans(dx, block_x, halo_x)
            sy, ry, cy = spans(dy, block_y, halo_y)
            copy = pltpu.make_async_remote_copy(
                src_ref=ref.at[pl.ds(sx, cx), pl.ds(sy, cy)],
                dst_ref=ref.at[pl.ds(rx, cx), pl.ds(ry, cy)],
                send_sem=send.at[turn, index],
                recv_sem=recv.at[turn, index],
                device_id=device(dx, dy),
                device_id_type=MESH,
            )
            copy.start()
            copies.append(copy)
        return copies

    def gather(slot):
        copies = []
        for d in range(1, gx):
            copy = pltpu.make_async_remote_copy(
                src_ref=G.at[slot, me_y, me_x],
                dst_ref=G.at[slot, me_y, me_x],
                send_sem=row_send.at[slot, d - 1],
                recv_sem=row_recv.at[slot, d - 1],
                device_id=device(d, 0),
                device_id_type=MESH,
            )
            copy.start()
            copies.append(copy)
        for copy in copies:
            copy.wait()
        copies = []
        for d in range(1, gy):
            copy = pltpu.make_async_remote_copy(
                src_ref=G.at[slot, me_y],
                dst_ref=G.at[slot, me_y],
                send_sem=col_send.at[slot, d - 1],
                recv_sem=col_recv.at[slot, d - 1],
                device_id=device(0, d),
                device_id_type=MESH,
            )
            copy.start()
            copies.append(copy)
        for copy in copies:
            copy.wait()

    own = density_ref[...]
    S[pl.ds(HALO, bx), pl.ds(HALO, by)] = own
    halo_copies = exchange(S, bx, HALO, by, HALO, near_send, near_recv, NEWTON - 1)
    part = jnp.sum(own, axis=0)
    tiles = part[0:8]
    for t in range(1, by // 8):
        tiles = tiles + part[8 * t : 8 * t + 8]
    G[NEWTON, me_y, me_x] = tiles
    U[...] = jnp.zeros_like(U)
    gather(NEWTON)
    mass = jnp.sum(G[NEWTON], axis=(0, 1))
    mass = jnp.sum(jnp.sum(mass, axis=0, keepdims=True), axis=1, keepdims=True)
    mean = mass / float(bx * gx * by * gy * nz)
    for copy in halo_copies:
        copy.wait()

    def to_source(i, carry):
        S[i] = S[i] / mean - 1.0
        return carry

    lax.fori_loop(0, bx + 2 * HALO, to_source, 0)

    L0 = Level(0, HALO, W0, T0, A0, B0)
    L1 = Level(1, pad1, W1, T1, A1, B1)
    L2 = Level(2, 2, W2, T2, A2, B2)
    L3 = Level(3, 2, W3, T3, A3, B3)

    lane_in = lax.broadcasted_iota(jnp.int32, (nz, nz), 0)
    lane_out = lax.broadcasted_iota(jnp.int32, (nz, nz), 1)
    width = nz // 4

    def dot(a, b):
        return lax.dot_general(
            a, b, (((1,), (0,)), ((), ())),
            precision=lax.Precision.HIGHEST, preferred_element_type=jnp.float32,
        )

    def newton(k, carry):
        L0.setup(U, 2, bx + 12, S)
        L0.half(A0, 3, bx + 10, False, store_to(B0))

        def leftover0(at, size):
            excess, _ = L0.excess(B0, at, size)
            R0[pl.ds(at // 2, size // 2)] = pair_xz(-excess, 1)

        planes(4, bx + 8, leftover0)
        pair_y(R0, 2, b1x + 4, by + 2 * HALO, T1, 2, row1 - pad1)

        def shrink0(at, size):
            R0[pl.ds(at // 2, size // 2)] = pair_xz(U[pl.ds(at, size)], 1)

        planes(0, bx + 2 * HALO, shrink0)
        pair_y(R0, 0, b1x + 2 * pad1, by + 2 * HALO, U1, 0, row1 - pad1)

        L1.setup(U1, 2, b1x + 4)
        L1.half(A1, 3, b1x + 2, False, store_to(B1))
        X1[pl.ds(pad1, b1x), pl.ds(row1, b1y)] = B1[pl.ds(pad1, b1x), pl.ds(row1, b1y)]
        mid_copies = exchange(X1, b1x, pad1, b1y, row1, mid_send, mid_recv, k)

        def leftover1(at, size):
            excess, _ = L1.excess(B1, at, size)
            R1[pl.ds((at - pad1) // 2, size // 2)] = pair_xz(-excess, 2)

        planes(pad1, b1x, leftover1)

        def shrink1(at, size):
            R1[pl.ds(b2x + (at - pad1) // 2, size // 2)] = pair_xz(U1[pl.ds(at, size)], 2)

        planes(pad1, b1x, shrink1)

        message = None
        for i in range(b2x):
            rows = []
            for which in range(2):
                low = R1[which * b2x + i, pl.ds(row1, b2y, stride=2), :]
                high = R1[which * b2x + i, pl.ds(row1 + 1, b2y, stride=2), :]
                rows.append((low + high) * 0.125)
            pick = ((lane_in & 3) == 0) & ((lane_in >> 2) + i * width == lane_out)
            term = dot(jnp.concatenate(rows, axis=0), pick.astype(jnp.float32))
            message = term if message is None else message + term
        G[k, me_y, me_x] = message
        gather(k)

        packed = G[k].reshape(gy * gx * 2 * b2y, nz)
        rights, fields = [], []
        for i in range(b2x):
            spread = (lane_in == (lane_out >> 2) + i * width).astype(jnp.float32)
            cells = dot(packed, spread).reshape(gy, gx, 2 * b2y, nz)
            rights.append(jnp.concatenate([cells[j, :, :b2y] for j in range(gy)], axis=1))
            fields.append(jnp.concatenate([cells[j, :, b2y:] for j in range(gy)], axis=1))
        T2[pl.ds(2, n2x)] = jnp.stack(rights, axis=1).reshape(n2x, n2y, nz)
        U2[pl.ds(2, n2x)] = jnp.stack(fields, axis=1).reshape(n2x, n2y, nz)
        wrap_planes(U2, 2, n2x)

        L2.setup(U2, 2, n2x)
        wrap_planes(A2, 2, n2x)
        L2.half(A2, 2, n2x, False, store_to(B2))
        wrap_planes(B2, 2, n2x)

        def leftover2(at, size):
            excess, _ = L2.excess(B2, at, size)
            R2[pl.ds((at - 2) // 2, size // 2)] = pair_xz(-excess, 4)

        planes(2, n2x, leftover2)
        pair_y(R2, 0, n3x, n2y, T3, 2, 0)

        def shrink2(at, size):
            R2[pl.ds((at - 2) // 2, size // 2)] = pair_xz(U2[pl.ds(at, size)], 4)

        planes(2, n2x, shrink2)
        pair_y(R2, 0, n3x, n2y, U3, 2, 0)
        wrap_planes(U3, 2, n3x)
        L3.setup(U3, 2, n3x)
        wrap_planes(A3, 2, n3x)
        L3.half(A3, 2, n3x, False, store_to(B3))
        wrap_planes(B3, 2, n3x)
        L3.half(B3, 2, n3x, True, store_to(A3))
        wrap_planes(A3, 2, n3x)
        L3.half(A3, 2, n3x, False, store_to(B3))

        def rise3(i, carry):
            value = B3[2 + i]
            R2[i, pl.ds(0, n3y, stride=2), :] = value
            R2[i, pl.ds(1, n3y, stride=2), :] = value
            both = R2[i]
            B2[2 + 2 * i] = B2[2 + 2 * i] + both
            B2[3 + 2 * i] = B2[3 + 2 * i] + both
            return carry

        lax.fori_loop(0, n3x, rise3, 0)
        wrap_planes(B2, 2, n2x)
        L2.half(B2, 2, n2x, True, store_to(A2))
        wrap_planes(A2, 2, n2x)
        L2.half(A2, 2, n2x, False, store_to(B2))
        wrap_planes(B2, 2, n2x)

        for copy in mid_copies:
            copy.wait()
        near = b2y + 4
        shift = lax.rem(n2y - me_y * b2y + 2, n2y)

        def rise2(i, carry):
            value = pltpu.roll(B2[me_x * b2x + i], shift, 0)[:near]
            R1[0, pl.ds(row1 - pad1, near, stride=2), :] = value
            R1[0, pl.ds(row1 - pad1 + 1, near, stride=2), :] = value
            both = R1[0]
            A1[2 * i] = X1[2 * i] + both
            A1[2 * i + 1] = X1[2 * i + 1] + both
            return carry

        lax.fori_loop(0, b2x + 4, rise2, 0)
        L1.half(A1, 2, b1x + 4, True, store_to(B1))
        L1.half(B1, 3, b1x + 2, False, store_to(A1))

        def rise1(i, carry):
            value = A1[i, pl.ds(row1 - pad1, b1y + 2 * pad1), :]
            R0[i, pl.ds(0, b1y + 2 * pad1, stride=2), :] = value
            R0[i, pl.ds(1, b1y + 2 * pad1, stride=2), :] = value
            both = R0[i]
            B0[2 * i] = B0[2 * i] + both
            B0[2 * i + 1] = B0[2 * i + 1] + both
            return carry

        lax.fori_loop(pad1 - 1, pad1 + b1x + 1, rise1, 0)
        L0.half(B0, HALO - 1, bx + 2, True, store_to(A0))

        def accept(at, size, value):
            where = (pl.ds(at, size), pl.ds(HALO, by))
            U[where] = U[where] + value[:, HALO : HALO + by]

        L0.half(A0, HALO, bx, False, accept)

        @pl.when(k < NEWTON - 1)
        def _():
            for copy in exchange(U, bx, HALO, by, HALO, near_send, near_recv, k):
                copy.wait()

        return carry

    lax.fori_loop(0, NEWTON, newton, 0)
    out_ref[...] = U[pl.ds(HALO, bx), pl.ds(HALO, by)]


def per_device(gx, gy, density):
    bx, by, nz = density.shape
    e0 = (bx + 2 * HALO, by + 2 * HALO, nz)
    e1 = (bx // 2 + HALO, by // 2 + 2 * HALO, nz)
    e2 = (bx // 4 * gx + 4, by // 4 * gy, nz)
    e3 = (bx // 8 * gx + 4, by // 8 * gy, nz)
    field = lambda shape: pltpu.VMEM(shape, jnp.float32)
    sems = lambda *shape: pltpu.SemaphoreType.DMA(shape)
    scratch = [field(e0), field(e0), field((7,) + e0)] + [field(e0)] * 3
    scratch += [field((e0[0] // 2,) + e0[1:])]
    scratch += [field(e1), field((7,) + e1)] + [field(e1)] * 4 + [field(e1)]
    scratch += [field(e2), field((7,) + e2)] + [field(e2)] * 3 + [field(e2)]
    scratch += [field(e3), field((7,) + e3)] + [field(e3)] * 3
    scratch += [field((NEWTON + 1, gy, gx, 8, nz))]
    scratch += [sems(NEWTON, 8)] * 4
    scratch += [sems(NEWTON + 1, gx - 1)] * 2 + [sems(NEWTON + 1, gy - 1)] * 2
    return pl.pallas_call(
        functools.partial(kernel, gx, gy),
        out_shape=jax.ShapeDtypeStruct(density.shape, jnp.float32),
        in_specs=[pl.BlockSpec(memory_space=pltpu.VMEM)],
        out_specs=pl.BlockSpec(memory_space=pltpu.VMEM),
        scratch_shapes=scratch,
        compiler_params=pltpu.CompilerParams(
            collective_id=0, has_side_effects=True, vmem_limit_bytes=60 * 2**20
        ),
    )(density)


def solution(mesh):
    placed = P("gx", "gy", None)
    return jax.shard_map(
        functools.partial(per_device, mesh.shape["gx"], mesh.shape["gy"]),
        mesh=mesh, in_specs=(placed,), out_specs=placed, check_vma=False,
    )
```

```python
import functools

import jax
import jax.numpy as jnp
from jax import lax
from jax.experimental import pallas as pl
from jax.experimental.pallas import tpu as pltpu
from jax.sharding import PartitionSpec as P

LEVELS = 4
NEWTON = 3
COUPLING = 0.1
FLOOR = 3.0
BLOCKS = 4
HALO = 8
MESH = pl.DeviceIdType.MESH


def parts_near(ref, at, size, row, rows, step, zero):
    def take(dx, dy):
        return ref[pl.ds(at + dx, size), pl.ds(zero + (row + dy), rows), :]

    lanes = ref.shape[2]

    def slope_z(value):
        return pltpu.roll(value, lanes - step, 2) - pltpu.roll(value, step, 2)

    center, x_next, x_prev = take(0, 0), take(1, 0), take(-1, 0)
    y_next, y_prev = take(0, 1), take(0, -1)
    twice = center + center
    xx = x_next + x_prev - twice
    yy = y_next + y_prev - twice
    zz = pltpu.roll(center, lanes - step, 2) + pltpu.roll(center, step, 2) - twice
    xy = take(1, 1) - take(1, -1) - take(-1, 1) + take(-1, -1)
    xz = slope_z(x_next - x_prev)
    yz = slope_z(y_next - y_prev)
    return center, xx, yy, zz, xy, xz, yz


def parts_whole(ref, at, size, step):
    block = ref[pl.ds(at - 1, size + 2)]
    rows, lanes = block.shape[1], block.shape[2]
    period = lanes // BLOCKS

    def z_pair(value):
        cell = lax.broadcasted_iota(jnp.int32, value.shape, 2) & (period - 1)
        forth = jnp.where(
            cell >= period - step,
            pltpu.roll(value, period - step, 2),
            pltpu.roll(value, lanes - step, 2),
        )
        back = jnp.where(
            cell < step,
            pltpu.roll(value, lanes - period + step, 2),
            pltpu.roll(value, step, 2),
        )
        return forth, back

    def slope_y(value):
        return pltpu.roll(value, rows - 1, 1) - pltpu.roll(value, 1, 1)

    center, x_next, x_prev = block[1:-1], block[2:], block[:-2]
    twice = center + center
    z_next, z_prev = z_pair(center)
    xx = x_next + x_prev - twice
    yy = pltpu.roll(center, rows - 1, 1) + pltpu.roll(center, 1, 1) - twice
    zz = z_next + z_prev - twice
    slope_x = x_next - x_prev
    forth, back = z_pair(slope_x)
    return center, xx, yy, zz, slope_y(slope_x), forth - back, slope_y(z_next - z_prev)


def red_of(shape, first, shift):
    total = (
        lax.broadcasted_iota(jnp.int32, shape, 0)
        + first
        + lax.broadcasted_iota(jnp.int32, shape, 1)
        + (lax.broadcasted_iota(jnp.int32, shape, 2) >> shift)
    )
    return (total & 1) == 0


def planes(first, count, body):
    size = 4 if count % 4 == 0 else 2
    assert count % size == 0

    def turn(i, carry):
        body(first + i * size, size)
        return carry

    lax.fori_loop(0, count // size, turn, 0)


class Level:
    def __init__(self, level, pad, whole, zero, weights, target, va, vb):
        self.level, self.pad, self.whole, self.zero = level, pad, whole, zero
        self.weights, self.target, self.va, self.vb = weights, target, va, vb
        self.shift = level - 2 if whole else level
        self.step = 1 << self.shift
        self.scale = 0.25**level

    def parts(self, ref, at, size, row, rows):
        if self.whole:
            return parts_whole(ref, at, size, self.step)
        return parts_near(ref, at, size, row, rows, self.step, self.zero)

    def at_rows(self, at, size, row, rows):
        if self.whole:
            return (pl.ds(at, size),)
        return (pl.ds(at, size), pl.ds(self.zero + row, rows), slice(None))

    def setup(self, u_ref, first, count, row, rows, source_ref=None):
        def body(at, size):
            _, xx, yy, zz, xy, xz, yz = self.parts(u_ref, at, size, row, rows)
            if self.level > 0:
                xx, yy, zz = xx * self.scale, yy * self.scale, zz * self.scale
            quarter = 0.25 * self.scale
            xy, xz, yz = xy * quarter, xz * quarter, yz * quarter
            kx = 1.0 + 2.0 * COUPLING * (yy + zz)
            ky = 1.0 + 2.0 * COUPLING * (xx + zz)
            kz = 1.0 + 2.0 * COUPLING * (xx + yy)
            diagonal = jnp.maximum(2.0 * (kx + ky + kz), FLOOR)
            relax = 1.0 / (self.scale * diagonal)
            where = self.at_rows(at, size, row, rows)
            if source_ref is not None:
                cubic = 2.0 * (xx * yy + xx * zz + yy * zz - xy * xy - xz * xz - yz * yz)
                target = source_ref[where] - (xx + yy + zz + COUPLING * cubic)
                self.target[where] = target
            else:
                target = self.target[where]
            mixed = -4.0 * COUPLING * quarter
            self.weights[(0,) + where] = kx * self.scale
            self.weights[(1,) + where] = ky * self.scale
            self.weights[(2,) + where] = kz * self.scale
            self.weights[(3,) + where] = xy * mixed
            self.weights[(4,) + where] = xz * mixed
            self.weights[(5,) + where] = yz * mixed
            self.weights[(6,) + where] = relax
            red = red_of(target.shape, (first - self.pad + row) % 2, self.shift)
            self.va[where] = jnp.where(red, -target * relax, 0.0)

        planes(first, count, body)

    def excess(self, v_ref, at, size, row, rows):
        center, xx, yy, zz, xy, xz, yz = self.parts(v_ref, at, size, row, rows)
        where = self.at_rows(at, size, row, rows)
        w = lambda index: self.weights[(index,) + where]
        total = w(0) * xx + w(1) * yy + w(2) * zz
        total += w(3) * xy + w(4) * xz + w(5) * yz
        return total - self.target[where], center

    def half(self, src, first, count, row, rows, red, put):
        def body(at, size):
            excess, center = self.excess(src, at, size, row, rows)
            where = self.at_rows(at, size, row, rows)
            change = excess * self.weights[(6,) + where]
            mask = red_of(change.shape, (first - self.pad + row) % 2, self.shift)
            if red:
                value = jnp.where(mask, center + change, center)
            else:
                value = jnp.where(mask, center, center + change)
            put(where, value)

        planes(first, count, body)


def store_to(ref):
    def put(where, value):
        ref[where] = value

    return put


def pair_xz(value, step):
    size, rows, lanes = value.shape
    halves = value.reshape(size // 2, 2, rows, lanes)
    value = halves[:, 0] + halves[:, 1]
    lane = lax.broadcasted_iota(jnp.int32, value.shape, 2)
    other = jnp.where(
        (lane & step) == 0, pltpu.roll(value, lanes - step, 2), pltpu.roll(value, step, 2)
    )
    return value + other


def pair_y(tmp, first, count, rows, out, out_first, out_row):
    half = rows // 2

    def body(i, carry):
        low = tmp[first + i, pl.ds(0, half, stride=2), :]
        high = tmp[first + i, pl.ds(1, half, stride=2), :]
        out[out_first + i, pl.ds(out_row, half), :] = (low + high) * 0.125
        return carry

    lax.fori_loop(0, count, body, 0)


def wrap_planes(ref, count):
    lanes = ref.shape[2]
    ref[0] = pltpu.roll(ref[count], lanes // BLOCKS, 1)
    ref[count + 1] = pltpu.roll(ref[1], lanes - lanes // BLOCKS, 1)


def kernel(
    gx, gy, density_ref, out_ref,
    S, U, W0, T0, A0, B0, R0,
    U1, W1, T1, A1, B1, X1, R1,
    U2, W2, T2, A2, B2, R2,
    U3, W3, T3, A3, B3,
    G,
    near_send, near_recv, mid_send, mid_recv, row_send, row_recv, col_send, col_recv,
):
    bx, by, nz = density_ref.shape
    me_x, me_y = lax.axis_index("gx"), lax.axis_index("gy")
    pad1 = HALO // 2
    b1x, b1y = bx // 2, by // 2
    b2x, b2y = bx // 4, by // 4
    n2x, n2y = b2x * gx, b2y * gy
    p2, p3, n3y = n2x // BLOCKS, n2x // (2 * BLOCKS), n2y // 2
    ahead = gx // BLOCKS
    zero = lax.div(me_y, gy)
    row1 = HALO

    def device(dx, dy):
        return (lax.rem(me_x + dx + gx, gx), lax.rem(me_y + dy + gy, gy))

    around = [(dx, dy) for dx in (-1, 0, 1) for dy in (-1, 0, 1) if (dx, dy) != (0, 0)]
    friends = [device(d, 0) for d in range(1, gx)]
    friends += [device(0, d) for d in range(1, gy)]
    friends += [device(dx, dy) for dx, dy in around if dx and dy]
    barrier = pltpu.get_barrier_semaphore()
    for friend in friends:
        pl.semaphore_signal(barrier, inc=1, device_id=friend, device_id_type=MESH)
    pl.semaphore_wait(barrier, len(friends))

    def spans(d, block, halo):
        if d == 0:
            return (halo, halo, block)
        if d == 1:
            return (block, 0, halo)
        return (halo, block + halo, halo)

    def exchange(ref, block_x, halo_x, block_y, halo_y, send, recv, turn):
        copies = []
        for index, (dx, dy) in enumerate(around):
            sx, rx, cx = spans(dx, block_x, halo_x)
            sy, ry, cy = spans(dy, block_y, halo_y)
            copy = pltpu.make_async_remote_copy(
                src_ref=ref.at[pl.ds(sx, cx), pl.ds(sy, cy)],
                dst_ref=ref.at[pl.ds(rx, cx), pl.ds(ry, cy)],
                send_sem=send.at[turn, index],
                recv_sem=recv.at[turn, index],
                device_id=device(dx, dy),
                device_id_type=MESH,
            )
            copy.start()
            copies.append(copy)
        return copies

    def gather(slot):
        copies = []
        for d in range(1, gx):
            copy = pltpu.make_async_remote_copy(
                src_ref=G.at[slot, me_y, me_x],
                dst_ref=G.at[slot, me_y, me_x],
                send_sem=row_send.at[slot, d - 1],
                recv_sem=row_recv.at[slot, d - 1],
                device_id=device(d, 0),
                device_id_type=MESH,
            )
            copy.start()
            copies.append(copy)
        for copy in copies:
            copy.wait()
        copies = []
        for d in range(1, gy):
            copy = pltpu.make_async_remote_copy(
                src_ref=G.at[slot, me_y],
                dst_ref=G.at[slot, me_y],
                send_sem=col_send.at[slot, d - 1],
                recv_sem=col_recv.at[slot, d - 1],
                device_id=device(0, d),
                device_id_type=MESH,
            )
            copy.start()
            copies.append(copy)
        for copy in copies:
            copy.wait()

    own = density_ref[...]
    S[pl.ds(HALO, bx), pl.ds(HALO, by)] = own
    halo_copies = exchange(S, bx, HALO, by, HALO, near_send, near_recv, NEWTON - 1)
    part = jnp.sum(own, axis=0)
    tiles = part[0:8]
    for t in range(1, by // 8):
        tiles = tiles + part[8 * t : 8 * t + 8]
    G[NEWTON, me_y, me_x] = tiles
    U[...] = jnp.zeros_like(U)
    gather(NEWTON)
    mass = jnp.sum(G[NEWTON], axis=(0, 1))
    mass = jnp.sum(jnp.sum(mass, axis=0, keepdims=True), axis=1, keepdims=True)
    mean = mass / float(bx * gx * by * gy * nz)
    for copy in halo_copies:
        copy.wait()

    def to_source(i, carry):
        S[i] = S[i] / mean - 1.0
        return carry

    lax.fori_loop(0, bx + 2 * HALO, to_source, 0)

    L0 = Level(0, HALO, False, zero, W0, T0, A0, B0)
    L1 = Level(1, pad1, False, zero, W1, T1, A1, B1)
    L2 = Level(2, 1, True, zero, W2, T2, A2, B2)
    L3 = Level(3, 1, True, zero, W3, T3, A3, B3)

    lane_in = lax.broadcasted_iota(jnp.int32, (nz, nz), 0)
    lane_out = lax.broadcasted_iota(jnp.int32, (nz, nz), 1)
    width = nz // 4

    def dot(a, b):
        return lax.dot_general(
            a, b, (((1,), (0,)), ((), ())),
            precision=lax.Precision.HIGHEST, preferred_element_type=jnp.float32,
        )

    def newton(k, carry):
        L0.setup(U, 2, bx + 12, 2, by + 12, S)
        L0.half(A0, 3, bx + 10, 3, by + 10, False, store_to(B0))

        def leftover0(at, size):
            excess, _ = L0.excess(B0, at, size, 4, by + 8)
            R0[pl.ds(at // 2, size // 2), pl.ds(0, by + 8)] = pair_xz(-excess, 1)

        planes(4, bx + 8, leftover0)
        pair_y(R0, 2, b1x + 4, by + 8, T1, 2, row1 - 2)

        def shrink0(at, size):
            R0[pl.ds(at // 2, size // 2)] = pair_xz(U[pl.ds(at, size)], 1)

        planes(0, bx + 2 * HALO, shrink0)
        pair_y(R0, 0, b1x + 2 * pad1, by + 2 * HALO, U1, 0, row1 - pad1)

        L1.setup(U1, 2, b1x + 4, row1 - 2, b1y + 4)
        L1.half(A1, 3, b1x + 2, row1 - 1, b1y + 2, False, store_to(B1))
        X1[pl.ds(pad1, b1x), pl.ds(row1, b1y)] = B1[pl.ds(pad1, b1x), pl.ds(row1, b1y)]
        mid_copies = exchange(X1, b1x, pad1, b1y, row1, mid_send, mid_recv, k)

        def leftover1(at, size):
            excess, _ = L1.excess(B1, at, size, row1, b1y)
            R1[pl.ds((at - pad1) // 2, size // 2), pl.ds(row1, b1y)] = pair_xz(-excess, 2)

        planes(pad1, b1x, leftover1)

        def shrink1(at, size):
            R1[pl.ds(b2x + (at - pad1) // 2, size // 2)] = pair_xz(U1[pl.ds(at, size)], 2)

        planes(pad1, b1x, shrink1)

        message = None
        for i in range(b2x):
            rows = []
            for which in range(2):
                low = R1[which * b2x + i, pl.ds(row1, b2y, stride=2), :]
                high = R1[which * b2x + i, pl.ds(row1 + 1, b2y, stride=2), :]
                rows.append((low + high) * 0.125)
            pick = ((lane_in & 3) == 0) & ((lane_in >> 2) + i * width == lane_out)
            term = dot(jnp.concatenate(rows, axis=0), pick.astype(jnp.float32))
            message = term if message is None else message + term
        G[k, me_y, me_x] = message
        gather(k)

        group = lax.broadcasted_iota(jnp.int32, (gy, ahead, 2 * b2y, nz), 3) // width
        rights, fields = [], []
        for i in range(b2x):
            cells = None
            for block in range(BLOCKS):
                part = G[k, :, block * ahead : (block + 1) * ahead]
                turn = (block - i) * width % nz
                if turn:
                    part = pltpu.roll(part, turn, 3)
                cells = part if cells is None else jnp.where(group == block, part, cells)
            rights.append(jnp.concatenate([cells[j, :, :b2y] for j in range(gy)], axis=1))
            fields.append(jnp.concatenate([cells[j, :, b2y:] for j in range(gy)], axis=1))
        T2[pl.ds(1, p2)] = jnp.stack(rights, axis=1).reshape(p2, n2y, nz)
        U2[pl.ds(1, p2)] = jnp.stack(fields, axis=1).reshape(p2, n2y, nz)
        wrap_planes(U2, p2)

        L2.setup(U2, 1, p2, 0, n2y)
        wrap_planes(A2, p2)
        L2.half(A2, 1, p2, 0, n2y, False, store_to(B2))
        wrap_planes(B2, p2)

        def leftover2(at, size):
            excess, _ = L2.excess(B2, at, size, 0, n2y)
            R2[pl.ds((at - 1) // 2, size // 2)] = pair_xz(-excess, 1)

        planes(1, p2, leftover2)
        pair_y(R2, 0, p3, n2y, T3, 1, 0)

        def shrink2(at, size):
            R2[pl.ds((at - 1) // 2, size // 2)] = pair_xz(U2[pl.ds(at, size)], 1)

        planes(1, p2, shrink2)
        pair_y(R2, 0, p3, n2y, U3, 1, 0)
        wrap_planes(U3, p3)
        L3.setup(U3, 1, p3, 0, n3y)
        wrap_planes(A3, p3)
        L3.half(A3, 1, p3, 0, n3y, False, store_to(B3))
        wrap_planes(B3, p3)
        L3.half(B3, 1, p3, 0, n3y, True, store_to(A3))
        wrap_planes(A3, p3)
        L3.half(A3, 1, p3, 0, n3y, False, store_to(B3))

        for i in range(p3):
            value = B3[1 + i]
            R2[i, pl.ds(0, n3y, stride=2), :] = value
            R2[i, pl.ds(1, n3y, stride=2), :] = value
            both = R2[i]
            B2[1 + 2 * i] = B2[1 + 2 * i] + both
            B2[2 + 2 * i] = B2[2 + 2 * i] + both
        wrap_planes(B2, p2)
        L2.half(B2, 1, p2, 0, n2y, True, store_to(A2))
        wrap_planes(A2, p2)
        L2.half(A2, 1, p2, 0, n2y, False, store_to(B2))

        for copy in mid_copies:
            copy.wait()
        near = b2y + 4
        shift = lax.rem(n2y - me_y * b2y + 2, n2y)
        taken = []
        for i in range(b2x + 4):
            plane = lax.rem(me_x * b2x + (n2x - 2 + i), n2x)
            value = B2[1 + lax.rem(plane, p2)]
            value = pltpu.roll(value, shift, 0)[:near]
            taken.append(pltpu.roll(value, lax.rem(nz - lax.div(plane, p2) * width, nz), 1))
        spread = (lane_in == (lane_out >> 2)).astype(jnp.float32)
        taken = dot(jnp.concatenate(taken, axis=0), spread)
        for i in range(b2x + 4):
            value = taken[i * near : (i + 1) * near]
            R1[0, pl.ds(row1 - pad1, near, stride=2), :] = value
            R1[0, pl.ds(row1 - pad1 + 1, near, stride=2), :] = value
            both = R1[0]
            A1[2 * i] = X1[2 * i] + both
            A1[2 * i + 1] = X1[2 * i + 1] + both

        L1.half(A1, 2, b1x + 4, row1 - 2, b1y + 4, True, store_to(B1))
        L1.half(B1, 3, b1x + 2, row1 - 1, b1y + 2, False, store_to(A1))

        def rise1(i, carry):
            value = A1[i, pl.ds(row1 - pad1, b1y + 2 * pad1), :]
            R0[i, pl.ds(0, b1y + 2 * pad1, stride=2), :] = value
            R0[i, pl.ds(1, b1y + 2 * pad1, stride=2), :] = value
            both = R0[i]
            B0[2 * i] = B0[2 * i] + both
            B0[2 * i + 1] = B0[2 * i + 1] + both
            return carry

        lax.fori_loop(pad1 - 1, pad1 + b1x + 1, rise1, 0)
        L0.half(B0, HALO - 1, bx + 2, HALO - 1, by + 2, True, store_to(A0))

        def accept(where, value):
            U[where] = U[where] + value

        L0.half(A0, HALO, bx, HALO, by, False, accept)

        @pl.when(k < NEWTON - 1)
        def _():
            for copy in exchange(U, bx, HALO, by, HALO, near_send, near_recv, k):
                copy.wait()

        return carry

    lax.fori_loop(0, NEWTON, newton, 0)
    out_ref[...] = U[pl.ds(HALO, bx), pl.ds(HALO, by)]


def per_device(gx, gy, density):
    bx, by, nz = density.shape
    e0 = (bx + 2 * HALO, by + 2 * HALO, nz)
    e1 = (bx // 2 + HALO, by // 2 + 2 * HALO, nz)
    e2 = (bx // 4 * gx // BLOCKS + 2, by // 4 * gy, nz)
    e3 = (bx // 8 * gx // BLOCKS + 2, by // 8 * gy, nz)
    field = lambda shape: pltpu.VMEM(shape, jnp.float32)
    sems = lambda *shape: pltpu.SemaphoreType.DMA(shape)
    scratch = [field(e0), field(e0), field((7,) + e0)] + [field(e0)] * 3
    scratch += [field((e0[0] // 2,) + e0[1:])]
    scratch += [field(e1), field((7,) + e1)] + [field(e1)] * 4 + [field(e1)]
    scratch += [field(e2), field((7,) + e2)] + [field(e2)] * 3 + [field(e2)]
    scratch += [field(e3), field((7,) + e3)] + [field(e3)] * 3
    scratch += [field((NEWTON + 1, gy, gx, 8, nz))]
    scratch += [sems(NEWTON, 8)] * 4
    scratch += [sems(NEWTON + 1, gx - 1)] * 2 + [sems(NEWTON + 1, gy - 1)] * 2
    return pl.pallas_call(
        functools.partial(kernel, gx, gy),
        out_shape=jax.ShapeDtypeStruct(density.shape, jnp.float32),
        in_specs=[pl.BlockSpec(memory_space=pltpu.VMEM)],
        out_specs=pl.BlockSpec(memory_space=pltpu.VMEM),
        scratch_shapes=scratch,
        compiler_params=pltpu.CompilerParams(
            collective_id=0, has_side_effects=True, vmem_limit_bytes=60 * 2**20
        ),
    )(density)


def solution(mesh):
    placed = P("gx", "gy", None)
    return jax.shard_map(
        functools.partial(per_device, mesh.shape["gx"], mesh.shape["gy"]),
        mesh=mesh, in_specs=(placed,), out_specs=placed, check_vma=False,
    )
```

```python
import functools

import jax
import jax.numpy as jnp
from jax import lax
from jax.experimental import pallas as pl
from jax.experimental.pallas import tpu as pltpu
from jax.sharding import PartitionSpec as P

LEVELS = 4
NEWTON = 3
COUPLING = 0.1
FLOOR = 3.0
BLOCKS = 4
HALO = 8
MESH = pl.DeviceIdType.MESH


def parts_near(ref, at, size, row, rows, step, zero):
    def take(dx, dy):
        return ref[pl.ds(at + dx, size), pl.ds(zero + (row + dy), rows), :]

    lanes = ref.shape[2]

    def slope_z(value):
        return pltpu.roll(value, lanes - step, 2) - pltpu.roll(value, step, 2)

    center, x_next, x_prev = take(0, 0), take(1, 0), take(-1, 0)
    y_next, y_prev = take(0, 1), take(0, -1)
    twice = center + center
    xx = x_next + x_prev - twice
    yy = y_next + y_prev - twice
    zz = pltpu.roll(center, lanes - step, 2) + pltpu.roll(center, step, 2) - twice
    xy = take(1, 1) - take(1, -1) - take(-1, 1) + take(-1, -1)
    xz = slope_z(x_next - x_prev)
    yz = slope_z(y_next - y_prev)
    return center, xx, yy, zz, xy, xz, yz


def parts_whole(ref, at, size, step):
    block = ref[pl.ds(at - 1, size + 2)]
    rows, lanes = block.shape[1], block.shape[2]
    period = lanes // BLOCKS

    def z_pair(value):
        cell = lax.broadcasted_iota(jnp.int32, value.shape, 2) & (period - 1)
        forth = jnp.where(
            cell >= period - step,
            pltpu.roll(value, period - step, 2),
            pltpu.roll(value, lanes - step, 2),
        )
        back = jnp.where(
            cell < step,
            pltpu.roll(value, lanes - period + step, 2),
            pltpu.roll(value, step, 2),
        )
        return forth, back

    def slope_y(value):
        return pltpu.roll(value, rows - 1, 1) - pltpu.roll(value, 1, 1)

    center, x_next, x_prev = block[1:-1], block[2:], block[:-2]
    twice = center + center
    z_next, z_prev = z_pair(center)
    xx = x_next + x_prev - twice
    yy = pltpu.roll(center, rows - 1, 1) + pltpu.roll(center, 1, 1) - twice
    zz = z_next + z_prev - twice
    slope_x = x_next - x_prev
    forth, back = z_pair(slope_x)
    return center, xx, yy, zz, slope_y(slope_x), forth - back, slope_y(z_next - z_prev)


def red_of(shape, first, shift):
    total = (
        lax.broadcasted_iota(jnp.int32, shape, 0)
        + first
        + lax.broadcasted_iota(jnp.int32, shape, 1)
        + (lax.broadcasted_iota(jnp.int32, shape, 2) >> shift)
    )
    return (total & 1) == 0


def planes(first, count, body):
    size = 4 if count % 4 == 0 else 2
    assert count % size == 0

    def turn(i, carry):
        body(first + i * size, size)
        return carry

    lax.fori_loop(0, count // size, turn, 0, unroll=True)


class Level:
    def __init__(self, level, pad, whole, zero, weights, target, va, vb):
        self.level, self.pad, self.whole, self.zero = level, pad, whole, zero
        self.weights, self.target, self.va, self.vb = weights, target, va, vb
        self.shift = level - 2 if whole else level
        self.step = 1 << self.shift
        self.scale = 0.25**level

    def parts(self, ref, at, size, row, rows):
        if self.whole:
            return parts_whole(ref, at, size, self.step)
        return parts_near(ref, at, size, row, rows, self.step, self.zero)

    def at_rows(self, at, size, row, rows):
        if self.whole:
            return (pl.ds(at, size),)
        return (pl.ds(at, size), pl.ds(self.zero + row, rows), slice(None))

    def setup(self, u_ref, first, count, row, rows, source_ref=None):
        def body(at, size):
            _, xx, yy, zz, xy, xz, yz = self.parts(u_ref, at, size, row, rows)
            if self.level > 0:
                xx, yy, zz = xx * self.scale, yy * self.scale, zz * self.scale
            quarter = 0.25 * self.scale
            xy, xz, yz = xy * quarter, xz * quarter, yz * quarter
            kx = 1.0 + 2.0 * COUPLING * (yy + zz)
            ky = 1.0 + 2.0 * COUPLING * (xx + zz)
            kz = 1.0 + 2.0 * COUPLING * (xx + yy)
            diagonal = jnp.maximum(2.0 * (kx + ky + kz), FLOOR)
            relax = 1.0 / (self.scale * diagonal)
            where = self.at_rows(at, size, row, rows)
            if source_ref is not None:
                cubic = 2.0 * (xx * yy + xx * zz + yy * zz - xy * xy - xz * xz - yz * yz)
                target = source_ref[where] - (xx + yy + zz + COUPLING * cubic)
                self.target[where] = target
            else:
                target = self.target[where]
            mixed = -4.0 * COUPLING * quarter
            self.weights[(0,) + where] = kx * self.scale
            self.weights[(1,) + where] = ky * self.scale
            self.weights[(2,) + where] = kz * self.scale
            self.weights[(3,) + where] = xy * mixed
            self.weights[(4,) + where] = xz * mixed
            self.weights[(5,) + where] = yz * mixed
            self.weights[(6,) + where] = relax
            red = red_of(target.shape, (first - self.pad + row) % 2, self.shift)
            self.va[where] = jnp.where(red, -target * relax, 0.0)

        planes(first, count, body)

    def excess(self, v_ref, at, size, row, rows):
        center, xx, yy, zz, xy, xz, yz = self.parts(v_ref, at, size, row, rows)
        where = self.at_rows(at, size, row, rows)
        w = lambda index: self.weights[(index,) + where]
        total = w(0) * xx + w(1) * yy + w(2) * zz
        total += w(3) * xy + w(4) * xz + w(5) * yz
        return total - self.target[where], center

    def half(self, src, first, count, row, rows, red, put):
        def body(at, size):
            excess, center = self.excess(src, at, size, row, rows)
            where = self.at_rows(at, size, row, rows)
            change = excess * self.weights[(6,) + where]
            mask = red_of(change.shape, (first - self.pad + row) % 2, self.shift)
            if red:
                value = jnp.where(mask, center + change, center)
            else:
                value = jnp.where(mask, center, center + change)
            put(where, value)

        planes(first, count, body)


def store_to(ref):
    def put(where, value):
        ref[where] = value

    return put


def pair_xz(value, step):
    size, rows, lanes = value.shape
    halves = value.reshape(size // 2, 2, rows, lanes)
    value = halves[:, 0] + halves[:, 1]
    lane = lax.broadcasted_iota(jnp.int32, value.shape, 2)
    other = jnp.where(
        (lane & step) == 0, pltpu.roll(value, lanes - step, 2), pltpu.roll(value, step, 2)
    )
    return value + other


def pair_y(tmp, first, count, rows, out, out_first, out_row):
    half = rows // 2

    def body(i, carry):
        low = tmp[first + i, pl.ds(0, half, stride=2), :]
        high = tmp[first + i, pl.ds(1, half, stride=2), :]
        out[out_first + i, pl.ds(out_row, half), :] = (low + high) * 0.125
        return carry

    lax.fori_loop(0, count, body, 0, unroll=True)


def wrap_planes(ref, count):
    lanes = ref.shape[2]
    ref[0] = pltpu.roll(ref[count], lanes // BLOCKS, 1)
    ref[count + 1] = pltpu.roll(ref[1], lanes - lanes // BLOCKS, 1)


def kernel(
    gx, gy, density_ref, out_ref,
    S, U, W0, T0, A0, B0, R0,
    U1, W1, T1, A1, B1, X1, R1,
    U2, W2, T2, A2, B2, R2,
    U3, W3, T3, A3, B3,
    G,
    near_send, near_recv, mid_send, mid_recv, row_send, row_recv, col_send, col_recv,
):
    bx, by, nz = density_ref.shape
    me_x, me_y = lax.axis_index("gx"), lax.axis_index("gy")
    pad1 = HALO // 2
    b1x, b1y = bx // 2, by // 2
    b2x, b2y = bx // 4, by // 4
    n2x, n2y = b2x * gx, b2y * gy
    p2, p3, n3y = n2x // BLOCKS, n2x // (2 * BLOCKS), n2y // 2
    ahead = gx // BLOCKS
    zero = lax.div(me_y, gy)
    row1 = HALO

    def device(dx, dy):
        return (lax.rem(me_x + dx + gx, gx), lax.rem(me_y + dy + gy, gy))

    around = [(dx, dy) for dx in (-1, 0, 1) for dy in (-1, 0, 1) if (dx, dy) != (0, 0)]
    friends = [device(d, 0) for d in range(1, gx)]
    friends += [device(0, d) for d in range(1, gy)]
    friends += [device(dx, dy) for dx, dy in around if dx and dy]
    barrier = pltpu.get_barrier_semaphore()
    for friend in friends:
        pl.semaphore_signal(barrier, inc=1, device_id=friend, device_id_type=MESH)
    pl.semaphore_wait(barrier, len(friends))

    def spans(d, block, halo):
        if d == 0:
            return (halo, halo, block)
        if d == 1:
            return (block, 0, halo)
        return (halo, block + halo, halo)

    def exchange(ref, block_x, halo_x, block_y, halo_y, send, recv, turn):
        copies = []
        for index, (dx, dy) in enumerate(around):
            sx, rx, cx = spans(dx, block_x, halo_x)
            sy, ry, cy = spans(dy, block_y, halo_y)
            copy = pltpu.make_async_remote_copy(
                src_ref=ref.at[pl.ds(sx, cx), pl.ds(sy, cy)],
                dst_ref=ref.at[pl.ds(rx, cx), pl.ds(ry, cy)],
                send_sem=send.at[turn, index],
                recv_sem=recv.at[turn, index],
                device_id=device(dx, dy),
                device_id_type=MESH,
            )
            copy.start()
            copies.append(copy)
        return copies

    def gather(slot):
        copies = []
        for d in range(1, gx):
            copy = pltpu.make_async_remote_copy(
                src_ref=G.at[slot, me_y, me_x],
                dst_ref=G.at[slot, me_y, me_x],
                send_sem=row_send.at[slot, d - 1],
                recv_sem=row_recv.at[slot, d - 1],
                device_id=device(d, 0),
                device_id_type=MESH,
            )
            copy.start()
            copies.append(copy)
        for copy in copies:
            copy.wait()
        copies = []
        for d in range(1, gy):
            copy = pltpu.make_async_remote_copy(
                src_ref=G.at[slot, me_y],
                dst_ref=G.at[slot, me_y],
                send_sem=col_send.at[slot, d - 1],
                recv_sem=col_recv.at[slot, d - 1],
                device_id=device(0, d),
                device_id_type=MESH,
            )
            copy.start()
            copies.append(copy)
        for copy in copies:
            copy.wait()

    own = density_ref[...]
    S[pl.ds(HALO, bx), pl.ds(HALO, by)] = own
    halo_copies = exchange(S, bx, HALO, by, HALO, near_send, near_recv, NEWTON - 1)
    part = jnp.sum(own, axis=0)
    tiles = part[0:8]
    for t in range(1, by // 8):
        tiles = tiles + part[8 * t : 8 * t + 8]
    G[NEWTON, me_y, me_x] = tiles
    U[...] = jnp.zeros_like(U)
    gather(NEWTON)
    mass = jnp.sum(G[NEWTON], axis=(0, 1))
    mass = jnp.sum(jnp.sum(mass, axis=0, keepdims=True), axis=1, keepdims=True)
    mean = mass / float(bx * gx * by * gy * nz)
    for copy in halo_copies:
        copy.wait()

    def to_source(i, carry):
        S[i] = S[i] / mean - 1.0
        return carry

    lax.fori_loop(0, bx + 2 * HALO, to_source, 0, unroll=4)

    L0 = Level(0, HALO, False, zero, W0, T0, A0, B0)
    L1 = Level(1, pad1, False, zero, W1, T1, A1, B1)
    L2 = Level(2, 1, True, zero, W2, T2, A2, B2)
    L3 = Level(3, 1, True, zero, W3, T3, A3, B3)

    lane_in = lax.broadcasted_iota(jnp.int32, (nz, nz), 0)
    lane_out = lax.broadcasted_iota(jnp.int32, (nz, nz), 1)
    width = nz // 4

    def dot(a, b):
        return lax.dot_general(
            a, b, (((1,), (0,)), ((), ())),
            precision=lax.Precision.HIGHEST, preferred_element_type=jnp.float32,
        )

    def newton(k, carry):
        L0.setup(U, 2, bx + 12, 2, by + 12, S)
        L0.half(A0, 3, bx + 10, 3, by + 10, False, store_to(B0))

        def leftover0(at, size):
            excess, _ = L0.excess(B0, at, size, 4, by + 8)
            R0[pl.ds(at // 2, size // 2), pl.ds(0, by + 8)] = pair_xz(-excess, 1)

        planes(4, bx + 8, leftover0)
        pair_y(R0, 2, b1x + 4, by + 8, T1, 2, row1 - 2)

        def shrink0(at, size):
            R0[pl.ds(at // 2, size // 2)] = pair_xz(U[pl.ds(at, size)], 1)

        planes(0, bx + 2 * HALO, shrink0)
        pair_y(R0, 0, b1x + 2 * pad1, by + 2 * HALO, U1, 0, row1 - pad1)

        L1.setup(U1, 2, b1x + 4, row1 - 2, b1y + 4)
        L1.half(A1, 3, b1x + 2, row1 - 1, b1y + 2, False, store_to(B1))
        X1[pl.ds(pad1, b1x), pl.ds(row1, b1y)] = B1[pl.ds(pad1, b1x), pl.ds(row1, b1y)]
        mid_copies = exchange(X1, b1x, pad1, b1y, row1, mid_send, mid_recv, k)

        def leftover1(at, size):
            excess, _ = L1.excess(B1, at, size, row1, b1y)
            R1[pl.ds((at - pad1) // 2, size // 2), pl.ds(row1, b1y)] = pair_xz(-excess, 2)

        planes(pad1, b1x, leftover1)

        def shrink1(at, size):
            R1[pl.ds(b2x + (at - pad1) // 2, size // 2)] = pair_xz(U1[pl.ds(at, size)], 2)

        planes(pad1, b1x, shrink1)

        message = None
        for i in range(b2x):
            rows = []
            for which in range(2):
                low = R1[which * b2x + i, pl.ds(row1, b2y, stride=2), :]
                high = R1[which * b2x + i, pl.ds(row1 + 1, b2y, stride=2), :]
                rows.append((low + high) * 0.125)
            pick = ((lane_in & 3) == 0) & ((lane_in >> 2) + i * width == lane_out)
            term = dot(jnp.concatenate(rows, axis=0), pick.astype(jnp.float32))
            message = term if message is None else message + term
        G[k, me_y, me_x] = message
        gather(k)

        group = lax.broadcasted_iota(jnp.int32, (gy, ahead, 2 * b2y, nz), 3) // width
        rights, fields = [], []
        for i in range(b2x):
            cells = None
            for block in range(BLOCKS):
                part = G[k, :, block * ahead : (block + 1) * ahead]
                turn = (block - i) * width % nz
                if turn:
                    part = pltpu.roll(part, turn, 3)
                cells = part if cells is None else jnp.where(group == block, part, cells)
            rights.append(jnp.concatenate([cells[j, :, :b2y] for j in range(gy)], axis=1))
            fields.append(jnp.concatenate([cells[j, :, b2y:] for j in range(gy)], axis=1))
        T2[pl.ds(1, p2)] = jnp.stack(rights, axis=1).reshape(p2, n2y, nz)
        U2[pl.ds(1, p2)] = jnp.stack(fields, axis=1).reshape(p2, n2y, nz)
        wrap_planes(U2, p2)

        L2.setup(U2, 1, p2, 0, n2y)
        wrap_planes(A2, p2)
        L2.half(A2, 1, p2, 0, n2y, False, store_to(B2))
        wrap_planes(B2, p2)

        def leftover2(at, size):
            excess, _ = L2.excess(B2, at, size, 0, n2y)
            R2[pl.ds((at - 1) // 2, size // 2)] = pair_xz(-excess, 1)

        planes(1, p2, leftover2)
        pair_y(R2, 0, p3, n2y, T3, 1, 0)

        def shrink2(at, size):
            R2[pl.ds((at - 1) // 2, size // 2)] = pair_xz(U2[pl.ds(at, size)], 1)

        planes(1, p2, shrink2)
        pair_y(R2, 0, p3, n2y, U3, 1, 0)
        wrap_planes(U3, p3)
        L3.setup(U3, 1, p3, 0, n3y)
        wrap_planes(A3, p3)
        L3.half(A3, 1, p3, 0, n3y, False, store_to(B3))
        wrap_planes(B3, p3)
        L3.half(B3, 1, p3, 0, n3y, True, store_to(A3))
        wrap_planes(A3, p3)
        L3.half(A3, 1, p3, 0, n3y, False, store_to(B3))

        for i in range(p3):
            value = B3[1 + i]
            R2[i, pl.ds(0, n3y, stride=2), :] = value
            R2[i, pl.ds(1, n3y, stride=2), :] = value
            both = R2[i]
            B2[1 + 2 * i] = B2[1 + 2 * i] + both
            B2[2 + 2 * i] = B2[2 + 2 * i] + both
        wrap_planes(B2, p2)
        L2.half(B2, 1, p2, 0, n2y, True, store_to(A2))
        wrap_planes(A2, p2)
        L2.half(A2, 1, p2, 0, n2y, False, store_to(B2))

        for copy in mid_copies:
            copy.wait()
        near = b2y + 4
        shift = lax.rem(n2y - me_y * b2y + 2, n2y)
        taken = []
        for i in range(b2x + 4):
            plane = lax.rem(me_x * b2x + (n2x - 2 + i), n2x)
            value = B2[1 + lax.rem(plane, p2)]
            value = pltpu.roll(value, shift, 0)[:near]
            taken.append(pltpu.roll(value, lax.rem(nz - lax.div(plane, p2) * width, nz), 1))
        spread = (lane_in == (lane_out >> 2)).astype(jnp.float32)
        taken = dot(jnp.concatenate(taken, axis=0), spread)
        for i in range(b2x + 4):
            value = taken[i * near : (i + 1) * near]
            R1[0, pl.ds(row1 - pad1, near, stride=2), :] = value
            R1[0, pl.ds(row1 - pad1 + 1, near, stride=2), :] = value
            both = R1[0]
            A1[2 * i] = X1[2 * i] + both
            A1[2 * i + 1] = X1[2 * i + 1] + both

        L1.half(A1, 2, b1x + 4, row1 - 2, b1y + 4, True, store_to(B1))
        L1.half(B1, 3, b1x + 2, row1 - 1, b1y + 2, False, store_to(A1))

        def rise1(i, carry):
            value = A1[i, pl.ds(row1 - pad1, b1y + 2 * pad1), :]
            R0[i, pl.ds(0, b1y + 2 * pad1, stride=2), :] = value
            R0[i, pl.ds(1, b1y + 2 * pad1, stride=2), :] = value
            both = R0[i]
            B0[2 * i] = B0[2 * i] + both
            B0[2 * i + 1] = B0[2 * i + 1] + both
            return carry

        lax.fori_loop(pad1 - 1, pad1 + b1x + 1, rise1, 0, unroll=True)
        L0.half(B0, HALO - 1, bx + 2, HALO - 1, by + 2, True, store_to(A0))

        def accept(where, value):
            U[where] = U[where] + value

        L0.half(A0, HALO, bx, HALO, by, False, accept)

        @pl.when(k < NEWTON - 1)
        def _():
            for copy in exchange(U, bx, HALO, by, HALO, near_send, near_recv, k):
                copy.wait()

        return carry

    lax.fori_loop(0, NEWTON, newton, 0)
    out_ref[...] = U[pl.ds(HALO, bx), pl.ds(HALO, by)]


def per_device(gx, gy, density):
    bx, by, nz = density.shape
    e0 = (bx + 2 * HALO, by + 2 * HALO, nz)
    e1 = (bx // 2 + HALO, by // 2 + 2 * HALO, nz)
    e2 = (bx // 4 * gx // BLOCKS + 2, by // 4 * gy, nz)
    e3 = (bx // 8 * gx // BLOCKS + 2, by // 8 * gy, nz)
    field = lambda shape: pltpu.VMEM(shape, jnp.float32)
    sems = lambda *shape: pltpu.SemaphoreType.DMA(shape)
    scratch = [field(e0), field(e0), field((7,) + e0)] + [field(e0)] * 3
    scratch += [field((e0[0] // 2,) + e0[1:])]
    scratch += [field(e1), field((7,) + e1)] + [field(e1)] * 4 + [field(e1)]
    scratch += [field(e2), field((7,) + e2)] + [field(e2)] * 3 + [field(e2)]
    scratch += [field(e3), field((7,) + e3)] + [field(e3)] * 3
    scratch += [field((NEWTON + 1, gy, gx, 8, nz))]
    scratch += [sems(NEWTON, 8)] * 4
    scratch += [sems(NEWTON + 1, gx - 1)] * 2 + [sems(NEWTON + 1, gy - 1)] * 2
    return pl.pallas_call(
        functools.partial(kernel, gx, gy),
        out_shape=jax.ShapeDtypeStruct(density.shape, jnp.float32),
        in_specs=[pl.BlockSpec(memory_space=pltpu.VMEM)],
        out_specs=pl.BlockSpec(memory_space=pltpu.VMEM),
        scratch_shapes=scratch,
        compiler_params=pltpu.CompilerParams(
            collective_id=0, has_side_effects=True, vmem_limit_bytes=60 * 2**20
        ),
    )(density)


def solution(mesh):
    placed = P("gx", "gy", None)
    return jax.shard_map(
        functools.partial(per_device, mesh.shape["gx"], mesh.shape["gy"]),
        mesh=mesh, in_specs=(placed,), out_specs=placed, check_vma=False,
    )
```
